256 devices in a mesh: groups: 4 (over x, y), head: 64 (over z, core).
Axes of the slice: x: 2, y: 2, z: 32, core: 2. Of those that a mesh axis runs over, the one named last changes fastest.
The devices are a block of a 4x8x32 slice.
Arguments:
- hidden_in: bfloat16 [2048, 3072], P(('groups', 'head')), parts along dimension 0, may hold values from -3 to 3
- queries: bfloat16 [2048, 6144], P(('groups', 'head')), parts along dimension 0, may hold values from -120 to 120, as said below
- keys: bfloat16 [2048, 512, 128], P(('groups', 'head')), parts along dimension 0, may hold values from -6 to 6
- values: bfloat16 [2048, 512, 128], P(('groups', 'head')), parts along dimension 0, may hold values from -6 to 6
- lengths: int32 [2048], P(('groups', 'head')), parts along dimension 0, may hold values from 1 to 64
- expert_ids: int32 [2048, 2], P('groups'), parts along dimension 0, may hold values from 0 to 3, all different within a row; in each aligned block of 8 rows (0 to 7, 8 to 15, ...) at most 6 rows name the same one
- w_out: bfloat16 [6144, 3072], P('head'), may hold values from -0.3125 to 0.3125
- norm_gain: bfloat16 [3072], replicated, may hold values from 0.5 to 1.5
- w_router: bfloat16 [3072, 4], replicated, may hold values from -0.21875 to 0.21875
- w_gate: bfloat16 [3072, 32768], P(None, 'head'), may hold values from -0.109375 to 0.109375
- w_up: bfloat16 [3072, 32768], P(None, 'head'), may hold values from -0.109375 to 0.109375
- w_down: bfloat16 [32768, 3072], P('head'), may hold values from -0.0625 to 0.0625
Outputs:
- layer_out: bfloat16 [2048, 3072], P(('groups', 'head')), parts along dimension 0
The draws below stay inside these ranges and needn't reach their ends.
There are 4 independent parts, one for each index of `groups`. The reference program is written for one: setup_inputs(seed, part) draws one part's arguments, and reference() takes and returns one part's arrays. A program takes and returns all parts, laid end to end along the dimension named above; an argument that names none is the same for every part. Nothing has to cross between parts.
Inputs may be any that keep to these rules, and one draw needn't show every extreme that they name: queries and keys are within -120 and 120. `expert_ids`: each row names 2 different experts; among the rows owned by one device no expert is named more than 6 times.
All inputs are finite; a program needn't handle non-finite values.
Results may differ from the reference program's by a relative error of at most 0.0057.
Values may be sent and summed in bfloat16 or wider, within the bound.
No kernel may reach another device: no remote copies, remote signals or barrier semaphores. Data moves between devices by JAX's collectives and lax.ppermute only.
A program may use at most 64 MiB of HBM per device.

```python
import math
import jax
import jax.numpy as jnp
import numpy as np
from jax import lax

D = 3072
H = 48
KV = 8
HD = 128
FF = 8192
EXPERTS = 4
TOP = 2
LEN = 64
TOK_DEV = 8
CAP = 6
TOKENS = 512
SHARDS = 16


def cache_keys(key):
    drawn = jax.random.normal(jax.random.fold_in(key, 11), (TOKENS, KV * LEN, HD), jnp.float32)
    return jnp.clip(drawn, -6.0, 6.0)


def draw_keys(key, part):
    return cache_keys(key).astype(jnp.bfloat16)


def draw_queries(key, part):
    drawn = jnp.clip(jax.random.normal(jax.random.fold_in(key, 12), (TOKENS, H * HD), jnp.float32), -6.0, 6.0)
    return drawn.astype(jnp.bfloat16)


def place_ends(entries, stream_key, low, largest):
    shape = entries.shape
    index_at = [jax.random.randint(jax.random.fold_in(stream_key, axis), (), 0, shape[axis]) for axis in range(len(shape))]
    entries = entries.at[tuple(index_at)].set(low)
    longest = shape.index(max(shape))
    index_at[longest] = (index_at[longest] + 1) % shape[longest]
    return entries.at[tuple(index_at)].set(largest)


def block_scale(own_key, extent, shards, smallest, high):
    factor_of, own = 1.0, jax.random.fold_in(own_key, 6)
    for position, shards_of in shards:
        steps = jnp.exp(jax.random.uniform(jax.random.fold_in(own, position), (shards_of,), jnp.float32, smallest / len(shards), high / len(shards)))
        factor_of = factor_of * jnp.repeat(steps, extent[position] // shards_of).reshape([-1 if axis == position else 1 for axis in range(len(extent))])
    return factor_of


def assign_block(stream_key, own, number, rows, number_of, top, reach, lean):
    order = jax.random.permutation(stream_key, number_of)
    packed, ordinary = portions_of(number_of, rows * top, reach, lean, True), portions_of(number_of, rows * top, reach, lean, False)
    places = jnp.arange(number_of)

    def named(sizes, offset_by):
        used = int((sizes > 0).sum())
        fixed = max(1, used // 4)
        moved = fixed + (places - fixed + offset_by * (used - fixed)) % max(1, number_of - fixed)
        return jnp.zeros((number_of,), jnp.int32).at[order[jnp.where(places < fixed, places, moved)]].set(jnp.asarray(sizes, jnp.int32))

    sizes = jnp.where(number % 4 == 0, named(packed, number // 4), named(ordinary, number - number // 4 - 1))
    mixed = jax.random.permutation(jax.random.fold_in(own, 3), number_of)
    giver, sink = mixed[0:number_of // 2 * 2:2], mixed[1:number_of // 2 * 2:2]
    slack = jnp.minimum(sizes[giver] - 1, reach - sizes[sink]) // 2
    slack = jnp.where((giver == order[0]) | (sink == order[0]) | (sizes[sink] == 0), 0, jnp.maximum(slack, 0))
    moved = jax.random.randint(jax.random.fold_in(own, 4), (number_of // 2,), 0, 1 << 20) % (slack + 1)
    sizes = sizes.at[giver].add(-moved).at[sink].add(moved)
    labels = jnp.searchsorted(jnp.cumsum(sizes), jnp.arange(rows * top), side="right").astype(jnp.int32)
    listing = labels.reshape(top, rows).T
    listing = listing[jax.random.permutation(jax.random.fold_in(own, 1), rows)]
    offset_by = jax.random.randint(jax.random.fold_in(own, 2), (rows, 1), 0, top)
    return jnp.take_along_axis(listing, (jnp.arange(top)[None, :] + offset_by) % top, axis=1)


def portions_of(amount, total, bound, slope, full):
    weights = [(1 << 20) // math.isqrt(standing ** slope) + 1 for standing in range(1, amount + 1)]
    largest = bound if full else min(bound, max(-(-total // amount), total * weights[0] // sum(weights)))
    least = 1 if total - largest >= amount - 1 else 0
    holding, spare = [largest] + [least] * (amount - 1), total - largest - least * (amount - 1)
    while spare > 0:
        candidates = [i for i in range(1, amount) if holding[i] < largest] or [i for i in range(1, amount) if holding[i] < bound]
        whole, remaining = sum([weights[i] for i in candidates]), spare
        for i in candidates:
            addition = min(bound - holding[i], max(1, remaining * weights[i] // whole), spare)
            holding[i] = holding[i] + addition
            spare = spare - addition
    return np.array(holding)


def noise(rng, dims, width, limit, split=(), kind=jnp.bfloat16):
    values = jax.random.normal(rng, dims, jnp.float32) * width
    if len(split) > 0:
        values = block_scale(rng, dims, split, -0.22, 0.18) * values
    return jnp.clip(values, min=-limit, max=limit).astype(kind)


def setup_inputs(seed: int = 0, part: int = 0) -> dict:
    arg_keys = jax.random.split(jax.random.key(seed), 13)
    part_keys = jax.random.split(jax.random.fold_in(arg_keys[12], part), 13)
    hidden_in = noise(part_keys[0], (TOKENS, D), 0.5, 3.0, ((0, 64),))
    queries = draw_queries(jax.random.fold_in(jax.random.fold_in(arg_keys[12], part), 71), part)
    keys = draw_keys(jax.random.fold_in(jax.random.fold_in(arg_keys[12], part), 71), part)
    values = noise(part_keys[3], (TOKENS, KV * LEN, HD), 1.0, 6.0, ((0, 64),))
    lengths = place_ends(jax.random.randint(part_keys[4], (TOKENS,), 1, LEN + 1), jax.random.fold_in(part_keys[4], 1), 1, LEN).astype(jnp.int32)
    expert_ids_keys = jax.random.split(jax.random.fold_in(part_keys[5], 1), TOKENS // TOK_DEV)
    expert_ids_turns = jax.random.permutation(jax.random.fold_in(part_keys[5], 3), TOKENS // TOK_DEV)
    expert_ids = jax.vmap(lambda own, number: assign_block(jax.random.fold_in(part_keys[5], 2), own, number, TOK_DEV, EXPERTS, TOP, CAP, 2))(expert_ids_keys, expert_ids_turns).reshape((TOKENS, TOP))
    w_out = noise(arg_keys[6], (H * HD, D), (H * HD // 16) ** -0.5, 0.3125, ((0, 64),))
    norm_gain = jnp.clip(1.0 + 0.1 * jax.random.normal(arg_keys[7], (D,), jnp.float32), 0.5, 1.5).astype(jnp.bfloat16)
    w_router = noise(arg_keys[8], (D, EXPERTS), (D // 4) ** -0.5, 0.21875)
    w_gate = noise(arg_keys[9], (D, EXPERTS * FF), D ** -0.5, 0.109375, ((1, 64),))
    w_up = noise(arg_keys[10], (D, EXPERTS * FF), D ** -0.5, 0.109375, ((1, 64),))
    w_down = noise(arg_keys[11], (EXPERTS * FF, D), FF ** -0.5, 0.0625, ((0, 64),))
    return dict(hidden_in=hidden_in, queries=queries, keys=keys, values=values, lengths=lengths, expert_ids=expert_ids, w_out=w_out, norm_gain=norm_gain, w_router=w_router, w_gate=w_gate, w_up=w_up, w_down=w_down)


EPSILON = 1e-05

def rms_scale(residual, norm_gain):
    mean_square = lax.optimization_barrier(jnp.mean(residual * residual, axis=-1, keepdims=True))
    return (residual * lax.rsqrt(mean_square + EPSILON) * norm_gain.astype(jnp.float32)).astype(jnp.bfloat16)

def gate_pair(logits, chosen_ids):
    marks = (chosen_ids[:, :, None] == jnp.arange(EXPERTS, dtype=jnp.int32)[None, None, :]).astype(jnp.float32)
    chosen = lax.optimization_barrier(jnp.sum(logits[:, None, :] * marks, axis=-1))
    first = jax.nn.sigmoid(chosen[:, 0] - chosen[:, 1])
    return jnp.stack([first, 1.0 - first], axis=1)

def reference(hidden_in, queries, keys, values, lengths, expert_ids, w_out, norm_gain, w_router, w_gate, w_up, w_down):
    ratio = H // KV
    query_all = queries.astype(jnp.float32).reshape(TOKENS, KV, ratio, HD)
    key_all = keys.astype(jnp.float32).reshape(TOKENS, KV, LEN, HD)
    value_all = values.astype(jnp.float32).reshape(TOKENS, KV, LEN, HD)
    scores = jnp.einsum('bgrd,bgld->bgrl', query_all, key_all) * HD ** (-0.5)
    live = (jnp.arange(LEN, dtype=jnp.int32)[None, :] < lengths[:, None])[:, None, None, :]
    scores = jnp.where(live, scores, -1e+30)
    peak = lax.optimization_barrier(jnp.max(scores, axis=-1, keepdims=True))
    weights = jnp.where(live, jnp.exp(scores - peak), 0.0)
    denominator = lax.optimization_barrier(jnp.sum(weights, axis=-1))
    probabilities = lax.optimization_barrier(weights.astype(jnp.bfloat16)).astype(jnp.float32)
    numerator = jnp.einsum('bgrl,bgld->bgrd', probabilities, value_all)
    attended = (numerator / denominator[..., None]).reshape(TOKENS, H * HD).astype(jnp.bfloat16)
    residual = hidden_in.astype(jnp.float32) + jnp.dot(attended, w_out, preferred_element_type=jnp.float32)
    normed = rms_scale(residual, norm_gain)
    logits = jnp.dot(normed, w_router, preferred_element_type=jnp.float32)
    gates = gate_pair(logits, expert_ids)
    piece = FF // SHARDS

    def expert_out(index):
        start = index * FF
        gate_cols = lax.dynamic_slice_in_dim(w_gate, start, FF, 1)
        up_cols = lax.dynamic_slice_in_dim(w_up, start, FF, 1)
        down_rows = lax.dynamic_slice_in_dim(w_down, start, FF, 0)
        gate_val = jnp.dot(normed, gate_cols, preferred_element_type=jnp.float32)
        up_val = jnp.dot(normed, up_cols, preferred_element_type=jnp.float32)
        hidden = (jax.nn.silu(gate_val) * up_val).astype(jnp.bfloat16)
        parts = jnp.einsum('bsf,sfd->bsd', hidden.astype(jnp.float32).reshape(TOKENS, SHARDS, piece), down_rows.astype(jnp.float32).reshape(SHARDS, piece, D))
        rounded = lax.optimization_barrier(parts.astype(jnp.bfloat16)).astype(jnp.float32)
        return lax.optimization_barrier(jnp.sum(rounded, axis=1))
    outputs = lax.map(expert_out, jnp.arange(EXPERTS, dtype=jnp.int32))
    marks = (expert_ids[:, :, None] == jnp.arange(EXPERTS, dtype=jnp.int32)[None, None, :]).astype(jnp.float32)
    mixture = jnp.einsum('bke,ebd->bd', gates[:, :, None] * marks, outputs, precision=lax.Precision.HIGHEST)
    return (residual + mixture).astype(jnp.bfloat16)
```

```python
import functools

import jax
import jax.numpy as jnp
from jax import lax
from jax.experimental import pallas as pl
from jax.experimental.pallas import tpu as pltpu
from jax.sharding import Mesh
from jax.sharding import PartitionSpec as P

H = 48
KV = 8
HD = 128
EXPERTS = 4
RING = "head_0"
CORE = "head_1"
HEAD = (RING, CORE)
GROUPS_HEAD = ("groups", "head_0", "head_1")


EPSILON = 1e-05


def rms_scale(residual, norm_gain):
    mean_square = jnp.mean(residual * residual, axis=-1, keepdims=True)
    return (residual * lax.rsqrt(mean_square + EPSILON) * norm_gain.astype(jnp.float32)).astype(
        jnp.bfloat16
    )


def gate_pair(logits, chosen_ids):
    marks = (chosen_ids[:, :, None] == jnp.arange(EXPERTS, dtype=jnp.int32)[None, None, :]).astype(
        jnp.float32
    )
    chosen = jnp.sum(logits[:, None, :] * marks, axis=-1)
    first = jax.nn.sigmoid(chosen[:, 0] - chosen[:, 1])
    return jnp.stack([first, 1.0 - first], axis=1)


def moved(x, distance):
    length = lax.axis_size(RING)
    return lax.ppermute(x, RING, [(i, (i + distance) % length) for i in range(length)])


def plan():
    length = lax.axis_size(RING)
    reach = (-(-length // 3)) // 2
    window = 2 * reach + 1
    assert 0 <= 3 * window - length <= 1
    return reach, window, 3 * window > length


def bundles():
    reach, window, doubled = plan()
    keys = [0] + [k for s in range(1, reach + 1) for k in (-s, s)]
    return {
        k: (k, k - window, k + window)[: 2 if doubled and k == reach else 3] for k in keys
    }


def gathered(own):
    reach, window, doubled = plan()
    rows = own.shape[0]
    behind, ahead = moved(own, window), moved(own, -window)
    right = left = jnp.concatenate([own, behind, ahead], axis=0)
    found = [right]
    for s in range(1, reach + 1):
        right = moved(right, 1)
        if doubled and s == reach:
            left = left[: 2 * rows]
        left = moved(left, -1)
        found += [right, left]
    return jnp.concatenate(found, axis=0)


def scattered(terms, rows):
    reach, window, _ = plan()
    start, at = {}, 0
    for k, offsets in bundles().items():
        start[k] = (at, at + len(offsets) * rows)
        at = start[k][1]

    def term(k):
        return lax.slice_in_dim(terms, *start[k], axis=0)

    def joined(received, own):
        rows = received.shape[0]
        if rows == own.shape[0]:
            return received.astype(jnp.float32) + own
        return jnp.concatenate([received.astype(jnp.float32) + own[:rows], own[rows:]], axis=0)

    right, left = term(reach), term(-reach)
    for s in range(reach, 0, -1):
        right_in = moved(right.astype(jnp.bfloat16), 1)
        left_in = moved(left.astype(jnp.bfloat16), -1)
        if s > 1:
            right = joined(right_in, term(s - 1))
            left = joined(left_in, term(1 - s))
    near = joined(right_in, term(0)) + left_in.astype(jnp.float32)
    from_ahead = moved(near[rows : 2 * rows].astype(jnp.bfloat16), -window)
    from_behind = moved(near[2 * rows :].astype(jnp.bfloat16), window)
    return near[:rows] + (from_ahead.astype(jnp.float32) + from_behind.astype(jnp.float32))


def experts_kernel(half, x, factor, gate, up, down, gate_too, up_too, down_too, out):
    step = pl.program_id(0)

    def add(gate_ref, up_ref, down_ref, first):
        gate_val = jnp.dot(x[...], gate_ref[...], preferred_element_type=jnp.float32)
        up_val = jnp.dot(x[...], up_ref[...], preferred_element_type=jnp.float32)
        hidden = (gate_val * jax.nn.sigmoid(gate_val) * up_val).astype(jnp.bfloat16)
        down_val = jnp.dot(hidden, down_ref[...], preferred_element_type=jnp.float32)
        out[...] = down_val if first else out[...] + down_val

    @pl.when(step == 0)
    def _():
        add(gate, up, down, True)

    @pl.when((step > 0) & (step < half))
    def _():
        add(gate, up, down, False)

    @pl.when(step >= half)
    def _():
        add(gate_too, up_too, down_too, False)

    @pl.when(step == 2 * half - 1)
    def _():
        out[...] = out[...] * factor[...]


def expert_terms(x, factor, own, partner):
    rows, width = x.shape
    units = own[0].shape[1]
    chunk = 256
    half = units // chunk
    early = lambda i: jnp.minimum(i, half - 1)
    late = lambda i: jnp.maximum(i - half, 0)

    def specs(which):
        return [
            pl.BlockSpec((width, chunk), lambda i: (0, which(i))),
            pl.BlockSpec((width, chunk), lambda i: (0, which(i))),
            pl.BlockSpec((chunk, width), lambda i: (which(i), 0)),
        ]

    return pl.pallas_call(
        functools.partial(experts_kernel, half),
        grid=(2 * half,),
        in_specs=[
            pl.BlockSpec((rows, width), lambda i: (0, 0)),
            pl.BlockSpec((rows, 1), lambda i: (0, 0)),
            *specs(early),
            *specs(late),
        ],
        out_specs=pl.BlockSpec((rows, width), lambda i: (0, 0)),
        out_shape=jax.ShapeDtypeStruct((rows, width), jnp.float32),
        compiler_params=pltpu.CompilerParams(
            dimension_semantics=("arbitrary",), vmem_limit_bytes=48 << 20
        ),
        cost_estimate=pl.CostEstimate(
            flops=12 * rows * width * units, bytes_accessed=12 * width * units, transcendentals=0
        ),
        name="experts",
    )(x, factor, *own, *partner)


def on_device(
    hidden_in,
    queries,
    keys,
    values,
    lengths,
    expert_ids,
    w_out,
    norm_gain,
    w_router,
    w_gate,
    w_up,
    w_down,
):
    length = lax.axis_size(RING)
    place = lax.axis_index(RING)
    core = lax.axis_index(CORE)
    cores = lax.axis_size(CORE)
    assert cores == 2

    def partners(x):
        return lax.ppermute(x, CORE, [(0, 1), (1, 0)])

    w_out_too = partners(w_out)
    w_gate_too, w_up_too, w_down_too = partners(w_gate), partners(w_up), partners(w_down)
    tok_rows, width = hidden_in.shape
    ratio = H // KV
    span = keys.shape[1] // KV
    my_queries = queries.reshape(tok_rows, KV, ratio, HD)
    my_keys = keys.reshape(tok_rows, KV, span, HD)
    my_values = values.reshape(tok_rows, KV, span, HD)
    scores = jnp.einsum(
        "bgrd,bgld->bgrl", my_queries, my_keys, preferred_element_type=jnp.float32
    ) * HD ** (-0.5)
    live = (jnp.arange(span, dtype=jnp.int32)[None, :] < lengths[:, None])[:, None, None, :]
    scores = jnp.where(live, scores, -1e30)
    peak = jnp.max(scores, axis=-1, keepdims=True)
    weights = jnp.where(live, jnp.exp(scores - peak), 0.0)
    denominator = jnp.sum(weights, axis=-1)
    numerator = jnp.einsum(
        "bgrl,bgld->bgrd",
        weights.astype(jnp.bfloat16),
        my_values,
        preferred_element_type=jnp.float32,
    )
    attended = (numerator / denominator[..., None]).reshape(tok_rows, H * HD).astype(jnp.bfloat16)
    column_block = lax.all_to_all(attended, RING, split_axis=1, concat_axis=0, tiled=True)

    order = [offset % length for offsets in bundles().values() for offset in offsets]
    assert sorted(order) == list(range(length))

    def in_order(x):
        x = jnp.roll(x, -place, axis=0)
        return jnp.concatenate([x[k : k + 1] for k in order], axis=0)

    column_block = in_order(column_block.reshape(length, tok_rows, -1)).reshape(
        length * tok_rows, -1
    )
    depth = w_out.shape[0]
    low, high = column_block[:, :depth], column_block[:, depth:]
    first = core == 0
    attn_terms = jnp.dot(
        jnp.where(first, low, high), w_out, preferred_element_type=jnp.float32
    ) + jnp.dot(jnp.where(first, high, low), w_out_too, preferred_element_type=jnp.float32)

    residual = hidden_in.astype(jnp.float32) + scattered(attn_terms, tok_rows)
    normed = rms_scale(residual, norm_gain)
    my_expert = place // (length // EXPERTS)
    piece = gathered(normed)
    ids = lax.dynamic_index_in_dim(
        expert_ids.reshape(length, cores, tok_rows, -1), core, axis=1, keepdims=False
    )
    ids = in_order(ids).reshape(length * tok_rows, -1)
    gates = gate_pair(jnp.dot(piece, w_router, preferred_element_type=jnp.float32), ids)
    factor = jnp.sum(gates * (ids == my_expert).astype(jnp.float32), axis=1)
    terms = expert_terms(
        piece, factor[:, None], (w_gate, w_up, w_down), (w_gate_too, w_up_too, w_down_too)
    )
    return (residual + scattered(terms, tok_rows)).astype(jnp.bfloat16)


def solution(mesh):
    cores = 2
    finer = Mesh(
        mesh.devices.reshape(mesh.shape["groups"], mesh.shape["head"] // cores, cores),
        GROUPS_HEAD,
    )
    return jax.shard_map(
        on_device,
        mesh=finer,
        in_specs=(
            P(GROUPS_HEAD, None),
            P(GROUPS_HEAD, None),
            P(GROUPS_HEAD, None, None),
            P(GROUPS_HEAD, None, None),
            P(GROUPS_HEAD),
            P("groups", None),
            P(HEAD, None),
            P(),
            P(),
            P(None, HEAD),
            P(None, HEAD),
            P(HEAD, None),
        ),
        out_specs=P(GROUPS_HEAD, None),
        check_vma=False,
    )
```

```python
import functools

import jax
import jax.numpy as jnp
from jax import lax
from jax.experimental import pallas as pl
from jax.experimental.pallas import tpu as pltpu
from jax.sharding import Mesh
from jax.sharding import PartitionSpec as P

H = 48
KV = 8
HD = 128
EXPERTS = 4
RING = "head_0"
CORE = "head_1"
HEAD = (RING, CORE)
GROUPS_HEAD = ("groups", "head_0", "head_1")


EPSILON = 1e-05
WEIGHT_REACH = 2


def outward(x):
    length = lax.axis_size(RING)
    pairs = [(2 * i, 2 * ((i - 1) % length)) for i in range(length)]
    pairs += [(2 * i + 1, 2 * ((i + 1) % length) + 1) for i in range(length)]
    return lax.ppermute(x, HEAD, pairs)


def projected(attended, w_out, slab):
    length = lax.axis_size(RING)
    place = lax.axis_index(RING)
    first = lax.axis_index(CORE) == 0
    rows = attended.shape[0]
    chip_depth = attended.shape[1] // length
    stride = 2 * WEIGHT_REACH + 1
    steps = -(-length // stride) // 2
    assert stride * (2 * steps + 1) >= length and steps >= WEIGHT_REACH

    doubled = jnp.concatenate([attended, attended], axis=1)
    turned = lax.dynamic_slice_in_dim(doubled, place * chip_depth, length * chip_depth, axis=1)
    taken, stretch = set(), {}
    for k in sorted(range(-steps, steps + 1), key=abs):
        pieces = []
        for n in range(-WEIGHT_REACH, WEIGHT_REACH + 1):
            chip = (k * stride + n) % length
            part = turned[:, chip * chip_depth : (chip + 1) * chip_depth]
            pieces.append(jnp.zeros_like(part) if chip in taken else part)
            taken.add(chip)
        stretch[k] = jnp.concatenate(pieces, axis=1)
    assert len(taken) == length
    right = jnp.concatenate([stretch[k] for k in range(1, steps + 1)], axis=0)
    left = jnp.concatenate([stretch[-k] for k in range(1, steps + 1)], axis=0)
    found = {0: stretch[0]}
    mine, theirs = [outward(slab)], []
    for k in range(1, steps + 1):
        right, left = moved(right, stride), moved(left, -stride)
        found[-k], found[k] = right[:rows], left[:rows]
        if k < WEIGHT_REACH:
            ready, _, _ = lax.optimization_barrier((mine[-1], right, left))
            mine.append(outward(ready))
            theirs.append(partner_of(ready))
        elif k == WEIGHT_REACH:
            theirs.append(partner_of(mine[-1]))
        right, left = right[rows:], left[rows:]
    order = range(-steps, steps + 1)
    block = jnp.concatenate([found[k] for k in order], axis=0)

    def columns(n):
        n += WEIGHT_REACH
        return block[:, n * chip_depth : (n + 1) * chip_depth]

    def product(x, w):
        return jnp.dot(x, w, preferred_element_type=jnp.float32)

    terms = product(columns(0), slab)
    for n in range(1, WEIGHT_REACH + 1):
        terms += product(jnp.where(first, columns(n), columns(-n)), mine[n - 1])
        terms += product(jnp.where(first, columns(-n), columns(n)), theirs[n - 1])

    def term(k):
        return lax.dynamic_slice_in_dim(terms, (k + steps) * rows, rows, axis=0)

    def step(i, carry):
        k = steps - 1 - i
        more = (k > 0).astype(jnp.float32)
        right = moved(carry[0].astype(jnp.bfloat16), stride).astype(jnp.float32)
        left = moved(carry[1].astype(jnp.bfloat16), -stride).astype(jnp.float32)
        return right + more * term(k), left + more * term(-k)

    right, left = lax.fori_loop(0, steps, step, (term(steps), term(-steps)))
    return term(0) + (right + left)


def rms_scale(residual, norm_gain):
    mean_square = jnp.mean(residual * residual, axis=-1, keepdims=True)
    return (residual * lax.rsqrt(mean_square + EPSILON) * norm_gain.astype(jnp.float32)).astype(
        jnp.bfloat16
    )


def gate_pair(logits, chosen_ids):
    marks = (chosen_ids[:, :, None] == jnp.arange(EXPERTS, dtype=jnp.int32)[None, None, :]).astype(
        jnp.float32
    )
    chosen = jnp.sum(logits[:, None, :] * marks, axis=-1)
    first = jax.nn.sigmoid(chosen[:, 0] - chosen[:, 1])
    return jnp.stack([first, 1.0 - first], axis=1)


def moved(x, distance):
    length = lax.axis_size(RING)
    return lax.ppermute(x, RING, [(i, (i + distance) % length) for i in range(length)])


def partner_of(x):
    return lax.ppermute(x, CORE, [(0, 1), (1, 0)])


def plan():
    length = lax.axis_size(RING)
    reach = (-(-length // 3)) // 2
    window = 2 * reach + 1
    assert 0 <= 3 * window - length <= 1
    return reach, window, 3 * window > length


def keys_in_order():
    reach, _, _ = plan()
    return [0] + [k for s in range(1, reach + 1) for k in (-s, s)]


def offsets_in_order():
    _, window, _ = plan()
    return [k + f for k in keys_in_order() for f in (0, -window, window)]


def gathered(own):
    reach, window, _ = plan()
    behind, ahead = moved(own, window), moved(own, -window)
    bundle = jnp.concatenate([own, behind, ahead], axis=0)
    rows = bundle.shape[0]
    found = [bundle]
    right = left = bundle
    for s in range(reach):
        right, left = moved(right, 1), moved(left, -1)
        found += [right, left]
    return jnp.concatenate(found, axis=0)


def scattered(terms, rows):
    reach, window, _ = plan()
    many = 3 * rows

    def term(at):
        return lax.dynamic_slice_in_dim(terms, at * many, many, axis=0)

    right, left = term(2 * reach), term(2 * reach - 1)
    right, left = right.astype(jnp.bfloat16), left.astype(jnp.bfloat16)

    def step(i, carry):
        s = reach - 1 - i
        right, left = moved(carry[0], 1), moved(carry[1], -1)
        right = (right.astype(jnp.float32) + term(2 * s)).astype(jnp.bfloat16)
        left = (left.astype(jnp.float32) + term(2 * s - 1)).astype(jnp.bfloat16)
        return right, left

    right, left = lax.fori_loop(0, reach - 1, step, (right, left))
    right, left = moved(right, 1), moved(left, -1)
    near = right.astype(jnp.float32) + left.astype(jnp.float32) + terms[:many]
    from_ahead = moved(near[rows : 2 * rows].astype(jnp.bfloat16), -window)
    from_behind = moved(near[2 * rows :].astype(jnp.bfloat16), window)
    return near[:rows] + (from_ahead.astype(jnp.float32) + from_behind.astype(jnp.float32))


def experts_kernel(half, x, factor, gate, up, down, gate_too, up_too, down_too, out):
    step = pl.program_id(0)

    def add(gate_ref, up_ref, down_ref):
        gate_val = jnp.dot(x[...], gate_ref[...], preferred_element_type=jnp.float32)
        up_val = jnp.dot(x[...], up_ref[...], preferred_element_type=jnp.float32)
        hidden = (gate_val * jax.nn.sigmoid(gate_val) * up_val).astype(jnp.bfloat16)
        down_val = jnp.dot(hidden, down_ref[...], preferred_element_type=jnp.float32)
        out[...] += down_val

    @pl.when(step == 0)
    def _():
        out[...] = jnp.zeros_like(out)

    @pl.when(step < half)
    def _():
        add(gate, up, down)

    @pl.when(step >= half)
    def _():
        add(gate_too, up_too, down_too)

    @pl.when(step == 2 * half - 1)
    def _():
        out[...] = out[...] * factor[...]


def expert_terms(x, factor, own, partner):
    rows, width = x.shape
    units = own[0].shape[1]
    chunk = 256
    half = units // chunk
    early = lambda i: jnp.minimum(i, half - 1)
    late = lambda i: jnp.maximum(i - half, 0)

    def specs(which):
        return [
            pl.BlockSpec((width, chunk), lambda i: (0, which(i))),
            pl.BlockSpec((width, chunk), lambda i: (0, which(i))),
            pl.BlockSpec((chunk, width), lambda i: (which(i), 0)),
        ]

    return pl.pallas_call(
        functools.partial(experts_kernel, half),
        grid=(2 * half,),
        in_specs=[
            pl.BlockSpec((rows, width), lambda i: (0, 0)),
            pl.BlockSpec((rows, 1), lambda i: (0, 0)),
            *specs(early),
            *specs(late),
        ],
        out_specs=pl.BlockSpec((rows, width), lambda i: (0, 0)),
        out_shape=jax.ShapeDtypeStruct((rows, width), jnp.float32),
        compiler_params=pltpu.CompilerParams(
            dimension_semantics=("arbitrary",), vmem_limit_bytes=48 << 20
        ),
        cost_estimate=pl.CostEstimate(
            flops=12 * rows * width * units, bytes_accessed=12 * width * units, transcendentals=0
        ),
        name="experts",
    )(x, factor, *own, *partner)


def on_device(
    hidden_in,
    queries,
    keys,
    values,
    lengths,
    expert_ids,
    w_out,
    norm_gain,
    w_router,
    w_gate,
    w_up,
    w_down,
):
    length = lax.axis_size(RING)
    place = lax.axis_index(RING)
    core = lax.axis_index(CORE)
    cores = lax.axis_size(CORE)
    assert cores == 2

    too = tuple(partner_of(w) for w in (w_gate, w_up, w_down))
    other = partner_of(w_out)
    first = core == 0
    slab = jnp.concatenate([jnp.where(first, w_out, other), jnp.where(first, other, w_out)], axis=0)
    slab, queries = lax.optimization_barrier((slab, queries))
    tok_rows, width = hidden_in.shape
    ratio = H // KV
    span = keys.shape[1] // KV
    my_queries = queries.reshape(tok_rows, KV, ratio, HD)
    my_keys = keys.reshape(tok_rows, KV, span, HD)
    my_values = values.reshape(tok_rows, KV, span, HD)
    scores = jnp.einsum(
        "bgrd,bgld->bgrl", my_queries, my_keys, preferred_element_type=jnp.float32
    ) * HD ** (-0.5)
    live = (jnp.arange(span, dtype=jnp.int32)[None, :] < lengths[:, None])[:, None, None, :]
    scores = jnp.where(live, scores, -1e30)
    peak = jnp.max(scores, axis=-1, keepdims=True)
    weights = jnp.where(live, jnp.exp(scores - peak), 0.0)
    denominator = jnp.sum(weights, axis=-1)
    numerator = jnp.einsum(
        "bgrl,bgld->bgrd",
        weights.astype(jnp.bfloat16),
        my_values,
        preferred_element_type=jnp.float32,
    )
    attended = (numerator / denominator[..., None]).reshape(tok_rows, H * HD).astype(jnp.bfloat16)
    order = offsets_in_order()
    seen = [offset % length for offset in order]
    once = [float(k not in seen[:i]) for i, k in enumerate(seen)]
    assert set(seen) == set(range(length))
    once = jnp.repeat(jnp.array(once, jnp.float32), tok_rows)[:, None]
    def in_order(x):
        x = jnp.roll(x, -place, axis=0)
        return jnp.concatenate([x[k : k + 1] for k in seen], axis=0).reshape(
            len(seen) * tok_rows, -1
        )

    residual = hidden_in.astype(jnp.float32) + projected(attended, w_out, slab)
    normed = rms_scale(residual, norm_gain)
    my_expert = place // (length // EXPERTS)
    piece = gathered(normed)
    ids = lax.dynamic_index_in_dim(
        expert_ids.reshape(length, cores, tok_rows, -1), core, axis=1, keepdims=False
    )
    ids = in_order(ids)
    gates = gate_pair(jnp.dot(piece, w_router, preferred_element_type=jnp.float32), ids)
    factor = jnp.sum(gates * (ids == my_expert).astype(jnp.float32), axis=1)
    factor = factor * once[:, 0]
    terms = expert_terms(
        piece, factor[:, None], (w_gate, w_up, w_down), too
    )
    return (residual + scattered(terms, tok_rows)).astype(jnp.bfloat16)


def solution(mesh):
    cores = 2
    finer = Mesh(
        mesh.devices.reshape(mesh.shape["groups"], mesh.shape["head"] // cores, cores),
        GROUPS_HEAD,
    )
    return jax.shard_map(
        on_device,
        mesh=finer,
        in_specs=(
            P(GROUPS_HEAD, None),
            P(GROUPS_HEAD, None),
            P(GROUPS_HEAD, None, None),
            P(GROUPS_HEAD, None, None),
            P(GROUPS_HEAD),
            P("groups", None),
            P(HEAD, None),
            P(),
            P(),
            P(None, HEAD),
            P(None, HEAD),
            P(HEAD, None),
        ),
        out_specs=P(GROUPS_HEAD, None),
        check_vma=False,
    )
```

```python
import functools

import jax
import jax.numpy as jnp
from jax import lax
from jax.experimental import pallas as pl
from jax.experimental.pallas import tpu as pltpu
from jax.sharding import Mesh
from jax.sharding import PartitionSpec as P

H = 48
KV = 8
HD = 128
EXPERTS = 4
RING = "head_0"
CORE = "head_1"
HEAD = (RING, CORE)
GROUPS_HEAD = ("groups", "head_0", "head_1")


EPSILON = 1e-05
WEIGHT_REACH = 2


def outward(x):
    length = lax.axis_size(RING)
    pairs = [(2 * i, 2 * ((i - 1) % length)) for i in range(length)]
    pairs += [(2 * i + 1, 2 * ((i + 1) % length) + 1) for i in range(length)]
    return lax.ppermute(x, HEAD, pairs)


def projected(attended, w_out, slab):
    length = lax.axis_size(RING)
    place = lax.axis_index(RING)
    first = lax.axis_index(CORE) == 0
    rows = attended.shape[0]
    chip_depth = attended.shape[1] // length
    stride = 2 * WEIGHT_REACH + 1
    steps = -(-length // stride) // 2
    assert stride * (2 * steps + 1) >= length and steps >= WEIGHT_REACH

    doubled = jnp.concatenate([attended, attended], axis=1)
    turned = lax.dynamic_slice_in_dim(doubled, place * chip_depth, length * chip_depth, axis=1)
    taken, stretch = set(), {}
    for k in sorted(range(-steps, steps + 1), key=abs):
        pieces = []
        for n in range(-WEIGHT_REACH, WEIGHT_REACH + 1):
            chip = (k * stride + n) % length
            part = turned[:, chip * chip_depth : (chip + 1) * chip_depth]
            pieces.append(jnp.zeros_like(part) if chip in taken else part)
            taken.add(chip)
        stretch[k] = jnp.concatenate(pieces, axis=1)
    assert len(taken) == length
    right = jnp.concatenate([stretch[k] for k in range(1, steps + 1)], axis=0)
    left = jnp.concatenate([stretch[-k] for k in range(1, steps + 1)], axis=0)
    found = {0: stretch[0]}
    mine, theirs = [outward(slab)], []
    for k in range(1, steps + 1):
        right, left = moved(right, stride), moved(left, -stride)
        found[-k], found[k] = right[:rows], left[:rows]
        if k < WEIGHT_REACH:
            ready = mine[-1]
            mine.append(outward(ready))
            theirs.append(partner_of(ready))
        elif k == WEIGHT_REACH:
            theirs.append(partner_of(mine[-1]))
        right, left = right[rows:], left[rows:]
    order = range(-steps, steps + 1)
    block = jnp.concatenate([found[k] for k in order], axis=0)

    def columns(n):
        n += WEIGHT_REACH
        return block[:, n * chip_depth : (n + 1) * chip_depth]

    def product(x, w):
        return jnp.dot(x, w, preferred_element_type=jnp.float32)

    terms = product(columns(0), slab)
    for n in range(1, WEIGHT_REACH + 1):
        terms += product(jnp.where(first, columns(n), columns(-n)), mine[n - 1])
        terms += product(jnp.where(first, columns(-n), columns(n)), theirs[n - 1])

    blocks = terms.reshape(-1, rows, terms.shape[1])

    def term(k):
        return lax.dynamic_index_in_dim(blocks, k + steps, axis=0, keepdims=False)

    def step(i, carry):
        k = steps - 1 - i
        more = (k > 0).astype(jnp.float32)
        right = moved(carry[0].astype(jnp.bfloat16), stride).astype(jnp.float32)
        left = moved(carry[1].astype(jnp.bfloat16), -stride).astype(jnp.float32)
        return right + more * term(k), left + more * term(-k)

    right, left = lax.fori_loop(0, steps, step, (term(steps), term(-steps)))
    return term(0) + (right + left)


def rms_scale(residual, norm_gain):
    mean_square = jnp.mean(residual * residual, axis=-1, keepdims=True)
    return (residual * lax.rsqrt(mean_square + EPSILON) * norm_gain.astype(jnp.float32)).astype(
        jnp.bfloat16
    )


def gate_pair(logits, chosen_ids):
    marks = (chosen_ids[:, :, None] == jnp.arange(EXPERTS, dtype=jnp.int32)[None, None, :]).astype(
        jnp.float32
    )
    chosen = jnp.sum(logits[:, None, :] * marks, axis=-1)
    first = jax.nn.sigmoid(chosen[:, 0] - chosen[:, 1])
    return jnp.stack([first, 1.0 - first], axis=1)


def moved(x, distance):
    length = lax.axis_size(RING)
    return lax.ppermute(x, RING, [(i, (i + distance) % length) for i in range(length)])


def partner_of(x):
    return lax.ppermute(x, CORE, [(0, 1), (1, 0)])


def plan():
    length = lax.axis_size(RING)
    reach = (-(-length // 3)) // 2
    window = 2 * reach + 1
    assert 0 <= 3 * window - length <= 1
    return reach, window, 3 * window > length


def keys_in_order():
    reach, _, _ = plan()
    return [0] + [k for s in range(1, reach + 1) for k in (-s, s)]


def offsets_in_order():
    _, window, _ = plan()
    return [k + f for k in keys_in_order() for f in (0, -window, window)]


def gathered(own):
    reach, window, _ = plan()
    behind, ahead = moved(own, window), moved(own, -window)
    bundle = jnp.concatenate([own, behind, ahead], axis=0)
    rows = bundle.shape[0]
    found = [bundle]
    right = left = bundle
    for s in range(reach):
        right, left = moved(right, 1), moved(left, -1)
        found += [right, left]
    return jnp.concatenate(found, axis=0)


def scattered(terms, rows):
    reach, window, _ = plan()
    many = 3 * rows
    bundled = terms.reshape(-1, many, terms.shape[1])

    def term(at):
        return lax.dynamic_index_in_dim(bundled, at, axis=0, keepdims=False)

    right, left = term(2 * reach), term(2 * reach - 1)
    right, left = right.astype(jnp.bfloat16), left.astype(jnp.bfloat16)

    def step(i, carry):
        s = reach - 1 - i
        right, left = moved(carry[0], 1), moved(carry[1], -1)
        right = (right.astype(jnp.float32) + term(2 * s)).astype(jnp.bfloat16)
        left = (left.astype(jnp.float32) + term(2 * s - 1)).astype(jnp.bfloat16)
        return right, left

    right, left = lax.fori_loop(0, reach - 1, step, (right, left))
    right, left = moved(right, 1), moved(left, -1)
    near = right.astype(jnp.float32) + left.astype(jnp.float32) + terms[:many]
    from_ahead = moved(near[rows : 2 * rows].astype(jnp.bfloat16), -window)
    from_behind = moved(near[2 * rows :].astype(jnp.bfloat16), window)
    return near[:rows] + (from_ahead.astype(jnp.float32) + from_behind.astype(jnp.float32))


def experts_kernel(half, x, factor, gate, up, down, gate_too, up_too, down_too, out):
    step = pl.program_id(0)

    def add(gate_ref, up_ref, down_ref):
        gate_val = jnp.dot(x[...], gate_ref[...], preferred_element_type=jnp.float32)
        up_val = jnp.dot(x[...], up_ref[...], preferred_element_type=jnp.float32)
        hidden = (gate_val * jax.nn.sigmoid(gate_val) * up_val).astype(jnp.bfloat16)
        down_val = jnp.dot(hidden, down_ref[...], preferred_element_type=jnp.float32)
        out[...] += down_val

    @pl.when(step == 0)
    def _():
        out[...] = jnp.zeros_like(out)

    @pl.when(step < half)
    def _():
        add(gate, up, down)

    @pl.when(step >= half)
    def _():
        add(gate_too, up_too, down_too)

    @pl.when(step == 2 * half - 1)
    def _():
        out[...] = out[...] * factor[...]


def expert_terms(x, factor, own, partner):
    rows, width = x.shape
    units = own[0].shape[1]
    chunk = 256
    half = units // chunk
    early = lambda i: jnp.minimum(i, half - 1)
    late = lambda i: jnp.maximum(i - half, 0)

    def specs(which):
        return [
            pl.BlockSpec((width, chunk), lambda i: (0, which(i))),
            pl.BlockSpec((width, chunk), lambda i: (0, which(i))),
            pl.BlockSpec((chunk, width), lambda i: (which(i), 0)),
        ]

    return pl.pallas_call(
        functools.partial(experts_kernel, half),
        grid=(2 * half,),
        in_specs=[
            pl.BlockSpec((rows, width), lambda i: (0, 0)),
            pl.BlockSpec((rows, 1), lambda i: (0, 0)),
            *specs(early),
            *specs(late),
        ],
        out_specs=pl.BlockSpec((rows, width), lambda i: (0, 0)),
        out_shape=jax.ShapeDtypeStruct((rows, width), jnp.float32),
        compiler_params=pltpu.CompilerParams(
            dimension_semantics=("arbitrary",), vmem_limit_bytes=48 << 20
        ),
        cost_estimate=pl.CostEstimate(
            flops=12 * rows * width * units, bytes_accessed=12 * width * units, transcendentals=0
        ),
        name="experts",
    )(x, factor, *own, *partner)


def on_device(
    hidden_in,
    queries,
    keys,
    values,
    lengths,
    expert_ids,
    w_out,
    norm_gain,
    w_router,
    w_gate,
    w_up,
    w_down,
):
    length = lax.axis_size(RING)
    place = lax.axis_index(RING)
    core = lax.axis_index(CORE)
    cores = lax.axis_size(CORE)
    assert cores == 2

    too = tuple(partner_of(w) for w in (w_gate, w_up, w_down))
    other = partner_of(w_out)
    first = core == 0
    slab = jnp.concatenate([jnp.where(first, w_out, other), jnp.where(first, other, w_out)], axis=0)
    slab, queries = lax.optimization_barrier((slab, queries))
    tok_rows, width = hidden_in.shape
    ratio = H // KV
    span = keys.shape[1] // KV
    my_queries = queries.reshape(tok_rows, KV, ratio, HD)
    my_keys = keys.reshape(tok_rows, KV, span, HD)
    my_values = values.reshape(tok_rows, KV, span, HD)
    scores = jnp.einsum(
        "bgrd,bgld->bgrl", my_queries, my_keys, preferred_element_type=jnp.float32
    ) * HD ** (-0.5)
    live = (jnp.arange(span, dtype=jnp.int32)[None, :] < lengths[:, None])[:, None, None, :]
    scores = jnp.where(live, scores, -1e30)
    peak = jnp.max(scores, axis=-1, keepdims=True)
    weights = jnp.where(live, jnp.exp(scores - peak), 0.0)
    denominator = jnp.sum(weights, axis=-1)
    numerator = jnp.einsum(
        "bgrl,bgld->bgrd",
        weights.astype(jnp.bfloat16),
        my_values,
        preferred_element_type=jnp.float32,
    )
    attended = (numerator / denominator[..., None]).reshape(tok_rows, H * HD).astype(jnp.bfloat16)
    order = offsets_in_order()
    seen = [offset % length for offset in order]
    once = [float(k not in seen[:i]) for i, k in enumerate(seen)]
    assert set(seen) == set(range(length))
    once = jnp.repeat(jnp.array(once, jnp.float32), tok_rows)[:, None]
    def in_order(x):
        x = jnp.roll(x, -place, axis=0)
        return jnp.concatenate([x[k : k + 1] for k in seen], axis=0).reshape(
            len(seen) * tok_rows, -1
        )

    residual = hidden_in.astype(jnp.float32) + projected(attended, w_out, slab)
    normed = rms_scale(residual, norm_gain)
    my_expert = place // (length // EXPERTS)
    piece = gathered(normed)
    ids = lax.dynamic_index_in_dim(
        expert_ids.reshape(length, cores, tok_rows, -1), core, axis=1, keepdims=False
    )
    ids = in_order(ids)
    gates = gate_pair(jnp.dot(piece, w_router, preferred_element_type=jnp.float32), ids)
    factor = jnp.sum(gates * (ids == my_expert).astype(jnp.float32), axis=1)
    factor = factor * once[:, 0]
    terms = expert_terms(
        piece, factor[:, None], (w_gate, w_up, w_down), too
    )
    return (residual + scattered(terms, tok_rows)).astype(jnp.bfloat16)


def solution(mesh):
    cores = 2
    finer = Mesh(
        mesh.devices.reshape(mesh.shape["groups"], mesh.shape["head"] // cores, cores),
        GROUPS_HEAD,
    )
    return jax.shard_map(
        on_device,
        mesh=finer,
        in_specs=(
            P(GROUPS_HEAD, None),
            P(GROUPS_HEAD, None),
            P(GROUPS_HEAD, None, None),
            P(GROUPS_HEAD, None, None),
            P(GROUPS_HEAD),
            P("groups", None),
            P(HEAD, None),
            P(),
            P(),
            P(None, HEAD),
            P(None, HEAD),
            P(HEAD, None),
        ),
        out_specs=P(GROUPS_HEAD, None),
        check_vma=False,
    )
```
